32 devices in a mesh: gx: 2 (over y), gy: 4 (over x, core), gz: 4 (over z).
Axes of the slice: x: 2, y: 2, z: 4, core: 2. Of those that a mesh axis runs over, the one named last changes fastest.
Arguments:
- targets: float32 [512, 512, 512], P('gx', 'gy', 'gz'), may hold values from -6 to 6
- basis_first: float32 [512, 512], replicated, may hold values from -0.25 to 0.25
- basis_second: float32 [512, 512], replicated, may hold values from -0.25 to 0.25
- basis_third: float32 [512, 512], replicated, may hold values from -0.25 to 0.25
- eigen_first: float32 [512], replicated, may hold values from 0.1 to 1
- eigen_second: float32 [512], replicated, may hold values from 0.1 to 1
- eigen_third: float32 [512], replicated, may hold values from 0.1 to 1
- noise: float32 [1], replicated, may hold values from 0.5 to 1
Outputs:
- weights: float32 [512, 512, 512], P('gx', 'gy', 'gz')
The draws below stay inside these ranges and needn't reach their ends.
All inputs are finite; a program needn't handle non-finite values.
Results may differ from the reference program's by a relative error of at most 0.000071.
Values sent between devices are 32-bit elements; how exact they have to be, the bound alone decides.
A program may use at most 128 MiB of HBM per device.

```python
import math
import jax
import jax.numpy as jnp
from jax import lax

N1 = 512
N2 = 512
N3 = 512


def steps_of(own_key, shape, shards, smallest, largest):
    def one(position, shards_of):
        heights = jax.random.uniform(jax.random.fold_in(jax.random.fold_in(own_key, 6), position), (shards_of,), jnp.float32, smallest / len(shards), largest / len(shards))
        return jnp.repeat(jnp.exp(heights), shape[position] // shards_of).reshape((-1,) + (1,) * (len(shape) - position - 1))

    loudness = one(*shards[0])
    for cut in shards[1:]:
        loudness = loudness * one(*cut)
    return loudness


def normal_values(stream_key, extent, spread, reach, split=(), kind=jnp.bfloat16):
    values = spread * jax.random.normal(stream_key, extent, jnp.float32)
    if split:
        values = values * steps_of(stream_key, extent, split, -0.22, 0.18)
    return jnp.clip(values, -reach, reach).astype(kind)


def setup_inputs(seed: int = 0) -> dict:
    streams_of = jax.random.split(jax.random.key(seed), 9)
    return {
        "targets": normal_values(streams_of[0], (N1, N2, N3), 1.0, 6.0, ((0, 2), (1, 4), (2, 4)), jnp.float32),
        "basis_first": normal_values(streams_of[1], (N1, N1), N1 ** -0.5, 0.25, (), jnp.float32),
        "basis_second": normal_values(streams_of[2], (N2, N2), N2 ** -0.5, 0.25, (), jnp.float32),
        "basis_third": normal_values(streams_of[3], (N3, N3), N3 ** -0.5, 0.25, (), jnp.float32),
        "eigen_first": jnp.clip(jnp.exp(jax.random.uniform(streams_of[4], (N1,), jnp.float32, math.log(0.1), math.log(1.0))), 0.1, 1.0),
        "eigen_second": jnp.clip(jnp.exp(jax.random.uniform(streams_of[5], (N2,), jnp.float32, math.log(0.1), math.log(1.0))), 0.1, 1.0),
        "eigen_third": jnp.clip(jnp.exp(jax.random.uniform(streams_of[6], (N3,), jnp.float32, math.log(0.1), math.log(1.0))), 0.1, 1.0),
        "noise": jnp.clip(jnp.exp(jax.random.uniform(streams_of[7], (1,), jnp.float32, math.log(0.5), math.log(1.0))), 0.5, 1.0),
    }


def reference(targets, basis_first, basis_second, basis_third, eigen_first, eigen_second, eigen_third, noise):
    high = lax.Precision.HIGHEST
    rotated = jnp.einsum('ijk,ia->ajk', targets, basis_first, precision=high)
    rotated = jnp.einsum('ajk,jb->abk', rotated, basis_second, precision=high)
    rotated = jnp.einsum('abk,kc->abc', rotated, basis_third, precision=high)
    spectrum = eigen_first[:, None, None] * eigen_second[None, :, None] * eigen_third[None, None, :] + noise[0]
    scaled = rotated / spectrum
    result = jnp.einsum('abc,kc->abk', scaled, basis_third, precision=high)
    result = jnp.einsum('abk,jb->ajk', result, basis_second, precision=high)
    result = jnp.einsum('ajk,ia->ijk', result, basis_first, precision=high)
    return result
```

```python
import jax
import jax.numpy as jnp
from jax import lax
from jax.experimental import pallas as pl
from jax.experimental.pallas import tpu as pltpu
from jax.sharding import PartitionSpec as P

MESH = pl.DeviceIdType.MESH
CHUNKS = 4
HIGH = lax.Precision.HIGH


def offsets_of(sizes, names):
    found = [{}]
    for name in names:
        found = [{**base, name: step} for base in found for step in range(sizes[name])]
    found = [one for one in found if any(one.values())]
    far = lambda one: min(one.get("gz", 0), sizes["gz"] - one.get("gz", 0))
    return sorted(found, key=lambda one: -far(one))


def kernel(sizes, tasks, n_in, fresh, *refs):
    ins, outs, sems = refs[:n_in], refs[n_in:-1 - 2 * len(tasks)], refs[-1 - 2 * len(tasks):]
    me = {name: lax.axis_index(name) for name in sizes}
    everyone = "gz" if any("gz" in task[1] for task in tasks) else ""
    reach = ("gz", "gx", "gy") if everyone else ("gx", "gy")
    shift = lambda off: {n: (lax.rem(me[n] + s, sizes[n]) if s else me[n]) for n, s in off.items()}

    barrier = pltpu.get_barrier_semaphore()
    greeted = offsets_of(sizes, reach)
    for off in greeted:
        pl.semaphore_signal(barrier, inc=1, device_id=shift(off), device_id_type=MESH)
    pl.semaphore_wait(barrier, len(greeted))

    def rank(where, names):
        total = 0
        for n in names:
            total = total * sizes[n] + where[n]
        return total

    def parts(task, source, target, where_from, where_to):
        gathers, names, first, depth = task[0], task[1], task[4], task[5]
        grid, spine = (target, source) if gathers else (source, target)
        holder = where_from if gathers else where_to
        other = where_to if gathers else where_from
        rows, cols = spine.shape[1], spine.shape[2]
        run = spine.shape[0] // max(1, _count(sizes, names))
        k_at = rank(other, names) * run + first
        spine_part = spine.at[pl.ds(k_at, depth)]
        row_at = pl.multiple_of(rank(holder, names[:-1]) * rows, 8)
        col_at = pl.multiple_of(rank(holder, names[-1:]) * cols, 128)
        grid_part = grid.at[:, pl.ds(row_at, rows), pl.ds(col_at, cols)]
        return (spine_part, grid_part) if gathers else (grid_part, spine_part)

    running = []
    for t, task in enumerate(tasks):
        source = ins[task[2]]
        target = outs[task[3]]
        send, recv = sems[2 * t], sems[2 * t + 1]
        for s, off in enumerate(offsets_of(sizes, task[1])):
            peer = shift(off)
            src, dst = parts(task, source, target, me, peer)
            copy = pltpu.make_async_remote_copy(
                src_ref=src, dst_ref=dst, send_sem=send.at[s], recv_sem=recv.at[s],
                device_id=peer, device_id_type=MESH,
            )
            copy.start()
            running.append(copy)
        src, dst = parts(task, source, target, me, me)
        own = pltpu.make_async_copy(src, dst, sems[-1].at[t])
        own.start()
        running.append(own)
    for copy in running:
        copy.wait()


def _count(sizes, names):
    total = 1
    for n in names:
        total *= sizes[n]
    return total


def exchange(sizes, cid, tasks, sources, shapes, carried=None):
    carried = carried or {}
    n_src = len(sources)
    aliases = {n_src + i: out for i, out in enumerate(sorted(carried))}
    extra = [carried[out] for out in sorted(carried)]
    scratch = []
    for task in tasks:
        n = _count(sizes, task[1]) - 1
        scratch += [pltpu.SemaphoreType.DMA((n,)), pltpu.SemaphoreType.DMA((n,))]
    scratch.append(pltpu.SemaphoreType.DMA((len(tasks),)))
    any_space = pl.BlockSpec(memory_space=pl.ANY)

    def body(*refs):
        kernel(sizes, tasks, n_src + len(extra), None, *refs)

    return pl.pallas_call(
        body,
        out_shape=[jax.ShapeDtypeStruct(s, jnp.float32) for s in shapes],
        in_specs=[any_space] * (n_src + len(extra)),
        out_specs=[any_space] * len(shapes),
        scratch_shapes=scratch,
        input_output_aliases=aliases,
        compiler_params=pltpu.CompilerParams(collective_id=cid, has_side_effects=True),
        name=f"exchange_{cid}",
    )(*sources, *extra)


def solution(mesh):
    sizes = {name: mesh.shape[name] for name in ("gx", "gy", "gz")}
    near, every = ("gx", "gy"), ("gz", "gx", "gy")

    def per_device(targets, b1, b2, b3, e1, e2, e3, noise):
        rows, cols, deep = targets.shape
        n1, n2, n3 = b1.shape[0], b2.shape[0], b3.shape[0]
        run = deep // _count(sizes, near)
        chunks = min(CHUNKS, run)
        part = run // chunks
        na, nb = n1 // _count(sizes, ("gz", "gx")), n2 // sizes["gy"]
        slab, whole, spine = (part, n1, n2), (n3, na, nb), (deep, rows, cols)
        lead = jnp.transpose(targets, (2, 0, 1))

        def forward(x):
            x = jnp.einsum("kij,jb->kib", x, b2, precision=HIGH)
            return jnp.einsum("ia,kib->kab", b1, x, precision=HIGH)

        def backward(x):
            x = jnp.einsum("kab,jb->kaj", x, b2, precision=HIGH)
            return jnp.einsum("ia,kaj->kij", b1, x, precision=HIGH)

        (x,) = exchange(sizes, 0, [(True, near, 0, 0, 0, part)], [lead], [slab])
        gathered = None
        for q in range(chunks):
            v = forward(x)
            tasks, sources, shapes = [(False, every, 0, 0, q * part, part)], [v], [whole]
            if q + 1 < chunks:
                tasks.append((True, near, 1, 1, (q + 1) * part, part))
                sources.append(lead)
                shapes.append(slab)
            got = exchange(sizes, 1 + q, tasks, sources, shapes, {} if gathered is None else {0: gathered})
            gathered = got[0]
            x = got[1] if q + 1 < chunks else None

        here = {n: lax.axis_index(n) for n in sizes}
        l1 = lax.dynamic_slice_in_dim(e1, (here["gz"] * sizes["gx"] + here["gx"]) * na, na, 0)
        l2 = lax.dynamic_slice_in_dim(e2, here["gy"] * nb, nb, 0)
        rotated = jnp.einsum("kab,kc->acb", gathered, b3, precision=HIGH)
        spectrum = l1[:, None, None] * l2[None, None, :] * e3[None, :, None] + noise[0]
        scaled = rotated / spectrum
        u = jnp.einsum("acb,kc->kab", scaled, b3, precision=HIGH)

        base = 1 + chunks
        (w,) = exchange(sizes, base, [(True, every, 0, 0, 0, part)], [u], [slab])
        result = None
        for q in range(chunks):
            y = backward(w)
            tasks, sources, shapes = [(False, near, 0, 0, q * part, part)], [y], [spine]
            if q + 1 < chunks:
                tasks.insert(0, (True, every, 1, 1, (q + 1) * part, part))
                sources.append(u)
                shapes.append(slab)
            got = exchange(sizes, base + 1 + q, tasks, sources, shapes, {} if result is None else {0: result})
            result = got[0]
            w = got[1] if q + 1 < chunks else None
        return jnp.transpose(result, (1, 2, 0))

    return jax.shard_map(
        per_device,
        mesh=mesh,
        in_specs=(P("gx", "gy", "gz"), P(), P(), P(), P(), P(), P(), P()),
        out_specs=P("gx", "gy", "gz"),
        check_vma=False,
    )
```
